32 devices in a mesh: dp: 8 (over y, x, core), seq: 4 (over z).
Axes of the slice: x: 2, y: 2, z: 4, core: 2. Of those that a mesh axis runs over, the one named last changes fastest.
Arguments:
- hidden_in: bfloat16 [8, 512, 2048], P('dp', 'seq'), may hold values from -6 to 6
- cotangent: bfloat16 [8, 512, 2048], P('dp', 'seq'), may hold values from -6 to 6
- norm_gain: float32 [2048], P('dp'), may hold values from 0.1 to 1.9
- route_weights: float32 [8, 512, 10], P('dp', 'seq'), may hold values from 0.1 to 1
- expert_ids: int32 [8, 512, 10], P('dp', 'seq'), may hold values from 0 to 63, all different within a row; in each aligned block of 128 rows (0 to 127, 128 to 255, ..., all dimensions but the last counted through in order) at most 24 rows name the same one
- expert_gate: bfloat16 [64, 2048, 512], P(('dp', 'seq')), may hold values from -0.125 to 0.125
- expert_up: bfloat16 [64, 2048, 512], P(('dp', 'seq')), may hold values from -0.125 to 0.125
- expert_down: bfloat16 [64, 512, 2048], P(('dp', 'seq')), may hold values from -0.25 to 0.25
Outputs:
- grad_hidden: bfloat16 [8, 512, 2048], P('dp', 'seq')
- grad_gain: float32 [2048], P('dp')
- grad_gate: bfloat16 [64, 2048, 512], P(('dp', 'seq'))
- grad_up: bfloat16 [64, 2048, 512], P(('dp', 'seq'))
- grad_down: bfloat16 [64, 512, 2048], P(('dp', 'seq'))
The draws below stay inside these ranges and needn't reach their ends.
Inputs may be any that keep to these rules, and one draw needn't show every extreme that they name: `expert_ids`: each token names 10 different experts. Among the rows of one device no expert is named by more than 24 of them, and in some device one expert is named by exactly 24.
All inputs are finite; a program needn't handle non-finite values.
Results may differ from the reference program's by a relative error of at most 0.0072.
Values may be sent and summed in bfloat16 or wider, within the bound.
No kernel may reach another device: no remote copies, remote signals or barrier semaphores. Data moves between devices by JAX's collectives and lax.ppermute only.
A program may use at most 192 MiB of HBM per device.

```python
import math
import jax
import jax.numpy as jnp
import numpy as np
from jax import lax

D = 2048
HIDDEN_SIZE = 512
TOP = 10
TOK_DEV = 128
SEQS = 8
LEN = 512
EXPERTS = 64
CAP = 24
N_DP = 8
N_SEQ = 4


def block_scale(key, dims, pieces, least, high):
    level = 1.0
    for axis_at, shards_of in pieces:
        draws = jax.random.uniform(jax.random.fold_in(jax.random.fold_in(key, 6), axis_at), (shards_of,), jnp.float32, least / len(pieces), high / len(pieces))
        level = level * jnp.repeat(jnp.exp(draws), dims[axis_at] // shards_of).reshape((-1,) + (1,) * (len(dims) - 1 - axis_at))
    return level


def shared_out(key, own, number, rows, amount, top, reach, slope):
    order = jax.random.permutation(key, amount)
    heavy_load, ordinary = portions_of(amount, rows * top, reach, slope, True), portions_of(amount, rows * top, reach, slope, False)
    places = jnp.arange(amount)

    def named(lengths, rotation):
        used = int((lengths > 0).sum())
        fixed = max(1, used // 4)
        shifted = fixed + (places - fixed + rotation * (used - fixed)) % max(1, amount - fixed)
        return jnp.zeros((amount,), jnp.int32).at[order[jnp.where(places < fixed, places, shifted)]].set(jnp.asarray(lengths, jnp.int32))

    lengths = jnp.where(number % 4 == 0, named(heavy_load, number // 4), named(ordinary, number - number // 4 - 1))
    mixed = jax.random.permutation(jax.random.fold_in(own, 3), amount)
    giver, sink = mixed[0:amount // 2 * 2:2], mixed[1:amount // 2 * 2:2]
    room = jnp.minimum(lengths[giver] - 1, reach - lengths[sink]) // 2
    room = jnp.where((giver == order[0]) | (sink == order[0]) | (lengths[sink] == 0), 0, jnp.maximum(room, 0))
    shifted = jax.random.randint(jax.random.fold_in(own, 4), (amount // 2,), 0, 1 << 20) % (room + 1)
    lengths = lengths.at[giver].add(-shifted).at[sink].add(shifted)
    members = jnp.searchsorted(jnp.cumsum(lengths), jnp.arange(rows * top), side="right").astype(jnp.int32)
    grid = members.reshape(top, rows).T
    grid = grid[jax.random.permutation(jax.random.fold_in(own, 1), rows)]
    rotation = jax.random.randint(jax.random.fold_in(own, 2), (rows, 1), 0, top)
    return jnp.take_along_axis(grid, (jnp.arange(top)[None, :] + rotation) % top, axis=1)


def portions_of(count, total, limit, skew, full):
    portions = [(1 << 20) // math.isqrt(rank ** skew) + 1 for rank in range(1, count + 1)]
    largest = limit if full else min(limit, max(-(-total // count), total * portions[0] // sum(portions)))
    least = 1 if total - largest >= count - 1 else 0
    given, rest = [largest] + [least] * (count - 1), total - largest - least * (count - 1)
    while rest > 0:
        candidates = [i for i in range(1, count) if given[i] < largest] or [i for i in range(1, count) if given[i] < limit]
        whole, left = sum([portions[i] for i in candidates]), rest
        for i in candidates:
            addition = min(limit - given[i], max(1, left * portions[i] // whole), rest)
            given[i] = given[i] + addition
            rest = rest - addition
    return np.array(given)


def normal_values(rng, shape, spread, bound, cuts=(), kind=jnp.bfloat16):
    array = jax.random.normal(rng, shape, jnp.float32) * spread
    if len(cuts) > 0:
        array = block_scale(rng, shape, cuts, -0.22, 0.18) * array
    return jnp.clip(array, min=-bound, max=bound).astype(kind)


def setup_inputs(seed: int = 0) -> dict:
    key_list = jax.random.split(jax.random.key(seed), 9)
    hidden_in = normal_values(key_list[0], (SEQS, LEN, D), 1.0, 6.0, ((0, 8), (1, 4)))
    cotangent = normal_values(key_list[1], (SEQS, LEN, D), 1.0, 6.0, ((0, 8), (1, 4)))
    norm_gain = jnp.clip(1.0 + 0.18 * jax.random.normal(key_list[2], (D,), jnp.float32), 0.1, 1.9)
    route_weights = jnp.clip(jnp.exp(math.log(1.0) - 2.3025851 * jax.random.uniform(key_list[3], (SEQS, LEN, TOP), jnp.float32) ** block_scale(key_list[3], (SEQS, LEN, TOP), ((0, 8), (1, 4)), -0.2, 0.2)), 0.1, 1.0)
    expert_ids_keys = jax.random.split(jax.random.fold_in(key_list[4], 1), SEQS * LEN // TOK_DEV)
    expert_ids_turns = jax.random.permutation(jax.random.fold_in(key_list[4], 3), SEQS * LEN // TOK_DEV)
    expert_ids = jax.vmap(lambda own, number: shared_out(jax.random.fold_in(key_list[4], 2), own, number, TOK_DEV, EXPERTS, TOP, CAP, 2))(expert_ids_keys, expert_ids_turns).reshape((SEQS, LEN, TOP))
    expert_gate = normal_values(key_list[5], (EXPERTS, D, HIDDEN_SIZE), D ** -0.5, 0.125, ((0, 32),))
    expert_up = normal_values(key_list[6], (EXPERTS, D, HIDDEN_SIZE), D ** -0.5, 0.125, ((0, 32),))
    expert_down = normal_values(key_list[7], (EXPERTS, HIDDEN_SIZE, D), HIDDEN_SIZE ** -0.5, 0.25, ((0, 32),))
    return dict(hidden_in=hidden_in, cotangent=cotangent, norm_gain=norm_gain, route_weights=route_weights, expert_ids=expert_ids, expert_gate=expert_gate, expert_up=expert_up, expert_down=expert_down)


EPSILON = 1e-06

def block_slots(block_experts):
    flat_experts = block_experts.reshape(-1)
    onehot = (flat_experts[:, None] == jnp.arange(EXPERTS, dtype=jnp.int32)[None, :]).astype(jnp.float32)
    before = jnp.cumsum(onehot, axis=0) - onehot
    earlier_count = lax.optimization_barrier(jnp.sum(before * onehot, axis=1)).astype(jnp.int32)
    return flat_experts * CAP + earlier_count

def reference(hidden_in, cotangent, norm_gain, route_weights, expert_ids, expert_gate, expert_up, expert_down):
    blocks = N_DP * N_SEQ
    model_width = hidden_in.shape[-1]
    per_block = TOK_DEV * TOP
    inputs = hidden_in.reshape(blocks * TOK_DEV, model_width).astype(jnp.float32)
    inverse_root = lax.rsqrt(lax.optimization_barrier(jnp.mean(inputs * inputs, axis=1, keepdims=True)) + EPSILON)
    scaled = inputs * inverse_root
    normed = (scaled * norm_gain[None, :]).astype(jnp.bfloat16)
    upstream = cotangent.reshape(blocks * TOK_DEV, model_width)
    weights_flat = route_weights.reshape(blocks * per_block)
    slot_index = lax.map(block_slots, expert_ids.reshape(blocks, TOK_DEV, TOP))

    def fill_table(block_slot):
        return jnp.zeros((EXPERTS * CAP,), jnp.int32).at[block_slot].set(jnp.arange(per_block, dtype=jnp.int32) + 1)
    slot_table = jax.vmap(fill_table)(slot_index)
    slot_table = slot_table.reshape(blocks, EXPERTS, CAP).transpose(1, 0, 2).reshape(EXPERTS, blocks * CAP)
    block_of_row = jnp.arange(blocks * CAP, dtype=jnp.int32) // CAP

    def one_expert(packed):
        slot_entry, gate_matrix, up_matrix, down_matrix = packed
        occupied = slot_entry > 0
        within = jnp.maximum(slot_entry - 1, 0)
        assignment = block_of_row * per_block + within
        token_row = block_of_row * TOK_DEV + within // TOP
        rows_in = jnp.where(occupied[:, None], normed[token_row], jnp.zeros((), jnp.bfloat16))
        row_weight = jnp.where(occupied, weights_flat[assignment], jnp.zeros((), jnp.float32))
        rows_grad = (row_weight[:, None] * upstream[token_row].astype(jnp.float32)).astype(jnp.bfloat16)
        pre_gate = jnp.dot(rows_in, gate_matrix, preferred_element_type=jnp.float32)
        pre_up = jnp.dot(rows_in, up_matrix, preferred_element_type=jnp.float32)
        sigmoid_gate = jax.nn.sigmoid(pre_gate)
        silu_gate = pre_gate * sigmoid_gate
        activation = (silu_gate * pre_up).astype(jnp.bfloat16)
        grad_act = jnp.dot(rows_grad, down_matrix.T, preferred_element_type=jnp.float32)
        gate_back = (grad_act * pre_up * sigmoid_gate * (1.0 + pre_gate * (1.0 - sigmoid_gate))).astype(jnp.bfloat16)
        up_back = (grad_act * silu_gate).astype(jnp.bfloat16)
        down_grad = jnp.dot(activation.T, rows_grad, preferred_element_type=jnp.float32).astype(jnp.bfloat16)
        gate_grad = jnp.dot(rows_in.T, gate_back, preferred_element_type=jnp.float32).astype(jnp.bfloat16)
        up_grad = jnp.dot(rows_in.T, up_back, preferred_element_type=jnp.float32).astype(jnp.bfloat16)
        returned = (jnp.dot(gate_back, gate_matrix.T, preferred_element_type=jnp.float32) + jnp.dot(up_back, up_matrix.T, preferred_element_type=jnp.float32)).astype(jnp.bfloat16)
        return (gate_grad, up_grad, down_grad, returned)
    grad_gate, grad_up, grad_down, returned = lax.map(one_expert, (slot_table, expert_gate, expert_up, expert_down))
    flat_back = returned.reshape(EXPERTS * blocks * CAP, model_width)

    def gather_block(packed):
        block_number, block_slot = packed
        where_rows = block_slot // CAP * (blocks * CAP) + block_number * CAP + block_slot % CAP
        picked = flat_back[where_rows].astype(jnp.float32).reshape(TOK_DEV, TOP, model_width)
        return lax.optimization_barrier(jnp.sum(picked, axis=1))
    summed = lax.map(gather_block, (jnp.arange(blocks, dtype=jnp.int32), slot_index))
    summed = summed.reshape(blocks * TOK_DEV, model_width)
    grad_gain = lax.optimization_barrier(jnp.sum(summed * scaled, axis=0))
    gained = summed * norm_gain[None, :]
    centered = lax.optimization_barrier(jnp.mean(gained * scaled, axis=1, keepdims=True))
    grad_hidden = (upstream.astype(jnp.float32) + inverse_root * (gained - scaled * centered)).astype(jnp.bfloat16)
    return (grad_hidden.reshape(hidden_in.shape), grad_gain, grad_gate, grad_up, grad_down)
```

```python
import jax
import jax.numpy as jnp
from jax import lax
from jax.sharding import PartitionSpec as P

TOP = 10


EPSILON = 1e-06

def shards(
    hidden_in, cotangent, norm_gain, route_weights, expert_ids, expert_gate, expert_up, expert_down
):
    tokens_here = hidden_in.shape[1]
    model_width = hidden_in.shape[2]
    local_experts = expert_gate.shape[0]
    dp_count = lax.axis_size("dp")
    seq_count = lax.axis_size("seq")
    devices = dp_count * seq_count
    expert_count = local_experts * devices
    capacity = max(2, tokens_here * TOP * 6 // (5 * expert_count))
    dp_at = lax.axis_index("dp")
    seq_at = lax.axis_index("seq")
    my_index = dp_at * seq_count + seq_at

    upstream = cotangent[0]
    all_grads = lax.all_gather(upstream, ("dp", "seq"), axis=0)

    gain_full = lax.all_gather(norm_gain, "dp", axis=0, tiled=True)
    inputs = hidden_in[0].astype(jnp.float32)
    inverse_root = lax.rsqrt(jnp.mean(inputs * inputs, axis=1, keepdims=True) + EPSILON)
    scaled = inputs * inverse_root
    normed = (scaled * gain_full[None, :]).astype(jnp.bfloat16)
    all_rows = lax.all_gather(normed, ("dp", "seq"), axis=0)

    ids_here = expert_ids[0]
    weights_here = route_weights[0]
    ids_all = lax.all_gather(ids_here.T, ("dp", "seq"), axis=0, tiled=False)
    weights_all = lax.all_gather(weights_here.T, ("dp", "seq"), axis=0, tiled=False)

    place = jnp.arange(tokens_here, dtype=jnp.int32)
    upper = (place[:, None] < place[None, :]).astype(jnp.bfloat16)
    slots = jnp.arange(capacity, dtype=jnp.int32)
    my_experts = my_index * local_experts + jnp.arange(local_experts, dtype=jnp.int32)

    named = ids_all[:, None, :, :] == my_experts[None, :, None, None]
    chosen = jnp.any(named, axis=2)
    weight = jnp.sum(jnp.where(named, weights_all[:, None, :, :], 0.0), axis=2)
    rank = jnp.einsum(
        "nit,tu->niu", chosen.astype(jnp.bfloat16), upper, preferred_element_type=jnp.float32
    ).astype(jnp.int32)
    picks = chosen[:, :, None, :] & (rank[:, :, None, :] == slots[None, None, :, None])
    row_weight = jnp.sum(jnp.where(picks, weight[:, :, None, :], 0.0), axis=3)
    picks = picks.reshape(devices, local_experts * capacity, tokens_here).astype(jnp.bfloat16)
    row_weight = row_weight.reshape(devices, local_experts * capacity, 1)

    def pick(table):
        return jnp.einsum("nst,ntd->nsd", picks, table, preferred_element_type=jnp.float32)

    four_shape = (devices, local_experts, capacity, model_width)
    rows_grad = (row_weight * pick(all_grads)).astype(jnp.bfloat16).reshape(four_shape)
    rows_in = pick(all_rows).astype(jnp.bfloat16).reshape(four_shape)

    grad_act = jnp.einsum(
        "nicd,ifd->nicf", rows_grad, expert_down, preferred_element_type=jnp.float32
    )
    pre_gate = jnp.einsum(
        "nicd,idf->nicf", rows_in, expert_gate, preferred_element_type=jnp.float32
    )
    pre_up = jnp.einsum("nicd,idf->nicf", rows_in, expert_up, preferred_element_type=jnp.float32)
    sigmoid_gate = jax.nn.sigmoid(pre_gate)
    silu_gate = pre_gate * sigmoid_gate
    activation = (silu_gate * pre_up).astype(jnp.bfloat16)
    gate_back = (grad_act * pre_up * sigmoid_gate * (1.0 + pre_gate * (1.0 - sigmoid_gate))).astype(
        jnp.bfloat16
    )
    up_back = (grad_act * silu_gate).astype(jnp.bfloat16)
    returned = (
        jnp.einsum("nicf,idf->nicd", gate_back, expert_gate, preferred_element_type=jnp.float32)
        + jnp.einsum("nicf,idf->nicd", up_back, expert_up, preferred_element_type=jnp.float32)
    ).astype(jnp.bfloat16)

    back_rows = lax.all_to_all(
        returned.reshape(devices, local_experts * capacity, model_width),
        ("dp", "seq"),
        split_axis=0,
        concat_axis=0,
        tiled=True,
    )

    grad_down = jnp.einsum(
        "nicf,nicd->ifd", activation, rows_grad, preferred_element_type=jnp.float32
    ).astype(jnp.bfloat16)
    grad_gate = jnp.einsum(
        "nicd,nicf->idf", rows_in, gate_back, preferred_element_type=jnp.float32
    ).astype(jnp.bfloat16)
    grad_up = jnp.einsum(
        "nicd,nicf->idf", rows_in, up_back, preferred_element_type=jnp.float32
    ).astype(jnp.bfloat16)

    experts_range = jnp.arange(expert_count, dtype=jnp.int32)
    chosen_here = jnp.any(
        ids_here[:, :, None] == experts_range[None, None, :], axis=1
    )
    rank_here = jnp.dot(
        upper.T, chosen_here.astype(jnp.bfloat16), preferred_element_type=jnp.float32
    ).astype(jnp.int32)
    sums = (
        chosen_here[:, :, None] & (rank_here[:, :, None] == slots[None, None, :])
    ).reshape(tokens_here, expert_count * capacity).astype(jnp.bfloat16)
    summed = jnp.dot(
        sums,
        back_rows.reshape(expert_count * capacity, model_width),
        preferred_element_type=jnp.float32,
    )
    local_gain = jnp.sum(summed * scaled, axis=0)
    total_gain = lax.psum(local_gain, ("dp", "seq"))
    shard_width = norm_gain.shape[0]
    grad_gain = lax.dynamic_slice(total_gain, (dp_at * shard_width,), (shard_width,))
    gained = summed * gain_full[None, :]
    centered = jnp.mean(gained * scaled, axis=1, keepdims=True)
    grad_hidden = (
        upstream.astype(jnp.float32) + inverse_root * (gained - scaled * centered)
    ).astype(jnp.bfloat16)
    return (grad_hidden.reshape(hidden_in.shape), grad_gain, grad_gate, grad_up, grad_down)


def solution(mesh):
    return jax.shard_map(
        shards,
        mesh=mesh,
        in_specs=(
            P("dp", "seq", None),
            P("dp", "seq", None),
            P("dp"),
            P("dp", "seq", None),
            P("dp", "seq", None),
            P(("dp", "seq"), None, None),
            P(("dp", "seq"), None, None),
            P(("dp", "seq"), None, None),
        ),
        out_specs=(
            P("dp", "seq", None),
            P("dp"),
            P(("dp", "seq"), None, None),
            P(("dp", "seq"), None, None),
            P(("dp", "seq"), None, None),
        ),
        check_vma=False,
    )
```

```python
import jax
import jax.numpy as jnp
from jax import lax
from jax.sharding import PartitionSpec as P

TOP = 10


EPSILON = 1e-06

HALVES = 2


def shards(
    hidden_in, cotangent, norm_gain, route_weights, expert_ids, expert_gate, expert_up, expert_down
):
    tokens_here = hidden_in.shape[1]
    model_width = hidden_in.shape[2]
    local_experts = expert_gate.shape[0]
    dp_count = lax.axis_size("dp")
    seq_count = lax.axis_size("seq")
    devices = dp_count * seq_count
    expert_count = local_experts * devices
    capacity = max(2, tokens_here * TOP * 6 // (5 * expert_count))
    dp_at = lax.axis_index("dp")
    seq_at = lax.axis_index("seq")
    my_index = dp_at * seq_count + seq_at

    upstream = cotangent[0]
    all_grads = lax.all_gather(upstream, ("dp", "seq"), axis=0)

    column = [hidden_in[0]] + [
        lax.ppermute(hidden_in[0], "seq", [(i, (i + j) % seq_count) for i in range(seq_count)])
        for j in range(1, seq_count)
    ]
    column = jnp.stack(column, axis=0)
    groups = dp_count // HALVES

    def hop(block, flip):
        return lax.ppermute(
            block,
            "dp",
            [(d, ((d // HALVES) ^ flip) * HALVES + d % HALVES) for d in range(dp_count)],
        )

    def swap(block):
        return lax.ppermute(block, "dp", [(d, d ^ 1) for d in range(dp_count)])

    if groups == 4:
        first = hop(column, 1)
        second = hop(column, 2)
        middle = seq_count // 2
        pieces = [
            column,
            first,
            second,
            hop(second[:middle], 1),
            hop(first[middle:], 2),
        ]
    else:
        pieces = [column] + [hop(column, flip) for flip in range(1, groups)]
    pieces = pieces + [swap(piece) for piece in pieces]

    group_at = dp_at // HALVES
    half_at = dp_at % HALVES
    order = jnp.arange(devices, dtype=jnp.int32)
    source = (
        ((group_at ^ (order // seq_count % groups)) * HALVES)
        + (half_at ^ (order // (seq_count * groups)))
    ) * seq_count + (seq_at - order % seq_count) % seq_count
    stands = (
        ((order // seq_count % HALVES) ^ half_at) * groups
        + ((order // (seq_count * HALVES)) ^ group_at)
    ) * seq_count + (seq_at - order % seq_count) % seq_count

    gain_full = lax.all_gather(norm_gain, "dp", axis=0, tiled=True)
    inputs = hidden_in[0].astype(jnp.float32)
    inverse_root = lax.rsqrt(jnp.mean(inputs * inputs, axis=1, keepdims=True) + EPSILON)
    scaled = inputs * inverse_root

    ids_here = expert_ids[0]
    weights_here = route_weights[0]
    ids_all = lax.all_gather(ids_here.T, ("dp", "seq"), axis=0, tiled=False)
    weights_all = lax.all_gather(weights_here.T, ("dp", "seq"), axis=0, tiled=False)

    place = jnp.arange(tokens_here, dtype=jnp.int32)
    upper = (place[:, None] < place[None, :]).astype(jnp.bfloat16)
    slots = jnp.arange(capacity, dtype=jnp.int32)
    my_experts = my_index * local_experts + jnp.arange(local_experts, dtype=jnp.int32)

    named = ids_all[:, None, :, :] == my_experts[None, :, None, None]
    chosen = jnp.any(named, axis=2)
    weight = jnp.sum(jnp.where(named, weights_all[:, None, :, :], 0.0), axis=2)
    rank = jnp.einsum(
        "nit,tu->niu", chosen.astype(jnp.bfloat16), upper, preferred_element_type=jnp.float32
    ).astype(jnp.int32)
    picks = chosen[:, :, None, :] & (rank[:, :, None, :] == slots[None, None, :, None])
    row_weight = jnp.sum(jnp.where(picks, weight[:, :, None, :], 0.0), axis=3)
    picks = picks.reshape(devices, local_experts * capacity, tokens_here).astype(jnp.bfloat16)
    row_weight = row_weight.reshape(devices, local_experts * capacity, 1)

    def pick(table):
        return jnp.einsum("nst,ntd->nsd", picks, table, preferred_element_type=jnp.float32)

    four_shape = (devices, local_experts, capacity, model_width)
    rows_grad = (row_weight * pick(all_grads)).astype(jnp.bfloat16).reshape(four_shape)
    rows_of = local_experts * capacity
    picks_moved = picks[source]
    picked = []
    start = 0
    for piece in pieces:
        stop = start + piece.shape[0]
        picked.append(
            jnp.einsum(
                "nst,ntd->nsd",
                picks_moved[start:stop],
                piece,
                preferred_element_type=jnp.float32,
            ).astype(jnp.bfloat16)
        )
        start = stop
    picked = jnp.concatenate(picked, axis=0).reshape(devices * rows_of, model_width)
    row_index = (stands[:, None] * rows_of + jnp.arange(rows_of, dtype=jnp.int32)).reshape(-1)
    arrived = picked[row_index].astype(jnp.float32)
    arrived_root = lax.rsqrt(jnp.mean(arrived * arrived, axis=1, keepdims=True) + EPSILON)
    rows_in = (arrived * arrived_root * gain_full[None, :]).astype(jnp.bfloat16)
    rows_in = rows_in.reshape(four_shape)

    grad_act = jnp.einsum(
        "nicd,ifd->nicf", rows_grad, expert_down, preferred_element_type=jnp.float32
    )
    pre_gate = jnp.einsum(
        "nicd,idf->nicf", rows_in, expert_gate, preferred_element_type=jnp.float32
    )
    pre_up = jnp.einsum("nicd,idf->nicf", rows_in, expert_up, preferred_element_type=jnp.float32)
    sigmoid_gate = jax.nn.sigmoid(pre_gate)
    silu_gate = pre_gate * sigmoid_gate
    activation = (silu_gate * pre_up).astype(jnp.bfloat16)
    gate_back = (grad_act * pre_up * sigmoid_gate * (1.0 + pre_gate * (1.0 - sigmoid_gate))).astype(
        jnp.bfloat16
    )
    up_back = (grad_act * silu_gate).astype(jnp.bfloat16)
    returned = (
        jnp.einsum("nicf,idf->nicd", gate_back, expert_gate, preferred_element_type=jnp.float32)
        + jnp.einsum("nicf,idf->nicd", up_back, expert_up, preferred_element_type=jnp.float32)
    ).astype(jnp.bfloat16)

    back_rows = lax.all_to_all(
        returned.reshape(devices, local_experts * capacity, model_width),
        ("dp", "seq"),
        split_axis=0,
        concat_axis=0,
        tiled=True,
    )

    grad_down = jnp.einsum(
        "nicf,nicd->ifd", activation, rows_grad, preferred_element_type=jnp.float32
    ).astype(jnp.bfloat16)
    grad_gate = jnp.einsum(
        "nicd,nicf->idf", rows_in, gate_back, preferred_element_type=jnp.float32
    ).astype(jnp.bfloat16)
    grad_up = jnp.einsum(
        "nicd,nicf->idf", rows_in, up_back, preferred_element_type=jnp.float32
    ).astype(jnp.bfloat16)

    experts_range = jnp.arange(expert_count, dtype=jnp.int32)
    chosen_here = jnp.any(
        ids_here[:, :, None] == experts_range[None, None, :], axis=1
    )
    rank_here = jnp.dot(
        upper.T, chosen_here.astype(jnp.bfloat16), preferred_element_type=jnp.float32
    ).astype(jnp.int32)
    sums = (
        chosen_here[:, :, None] & (rank_here[:, :, None] == slots[None, None, :])
    ).reshape(tokens_here, expert_count * capacity).astype(jnp.bfloat16)
    summed = jnp.dot(
        sums,
        back_rows.reshape(expert_count * capacity, model_width),
        preferred_element_type=jnp.float32,
    )
    local_gain = jnp.sum(summed * scaled, axis=0)
    total_gain = lax.psum(local_gain, ("dp", "seq"))
    shard_width = norm_gain.shape[0]
    grad_gain = lax.dynamic_slice(total_gain, (dp_at * shard_width,), (shard_width,))
    gained = summed * gain_full[None, :]
    centered = jnp.mean(gained * scaled, axis=1, keepdims=True)
    grad_hidden = (
        upstream.astype(jnp.float32) + inverse_root * (gained - scaled * centered)
    ).astype(jnp.bfloat16)
    return (grad_hidden.reshape(hidden_in.shape), grad_gain, grad_gate, grad_up, grad_down)


def solution(mesh):
    return jax.shard_map(
        shards,
        mesh=mesh,
        in_specs=(
            P("dp", "seq", None),
            P("dp", "seq", None),
            P("dp"),
            P("dp", "seq", None),
            P("dp", "seq", None),
            P(("dp", "seq"), None, None),
            P(("dp", "seq"), None, None),
            P(("dp", "seq"), None, None),
        ),
        out_specs=(
            P("dp", "seq", None),
            P("dp"),
            P(("dp", "seq"), None, None),
            P(("dp", "seq"), None, None),
            P(("dp", "seq"), None, None),
        ),
        check_vma=False,
    )
```
